512 devices in a mesh: seq: 64 (over z_hi, x, y), head: 8 (over z_lo, core).
Axes of the slice: x: 4, y: 8, z: 8 (z_hi: 2, z_lo: 4; z = z_hi * 4 + z_lo), core: 2. Of those that a mesh axis runs over, the one named last changes fastest.
Arguments:
- queries: bfloat16 [12288, 32, 128], P('seq', 'head'), may hold values from -180 to 180
- key_rows: bfloat16 [12288, 8, 128], P('seq', 'head'), may hold values from -4.5 to 4.5
- value_rows: bfloat16 [12288, 8, 128], P('seq', 'head'), may hold values from -24 to 24
- windows: int32 [32], P('head'), may hold values from 768 to 1536, as said below
- sink_counts: int32 [32], P('head'), may hold values from 1 to 4, as said below
- sink_bias: float32 [32], P('head'), may hold values from 3 to 7
- out_weight: bfloat16 [4096, 4096], P('head'), may hold values from -0.09375 to 0.09375
Outputs:
- attn_out: bfloat16 [12288, 4096], P(('seq', 'head'))
The draws below stay inside these ranges and needn't reach their ends.
Inputs may be any that keep to these rules, and one draw needn't show every extreme that they name: `windows`: each head's window lies between 768 and 1536, and some head has exactly 1536. `sink_counts`: each head has 1 to 4 sink tokens, and some head has exactly 4.
All inputs are finite; a program needn't handle non-finite values.
Results may differ from the reference program's by a relative error of at most 0.018.
Values may be sent and summed in bfloat16 or wider, within the bound.
A program may use at most 64 MiB of HBM per device.

```python
import jax
import jax.numpy as jnp
from jax import lax

D = 4096
H = 32
KVH = 8
HD = 128
WINDOW = 1536
SINKS = 4
TOK_DEV = 192
TOKENS = 12288
N_SEQ = 64
N_HEAD = 8


def shared_keys(key):
    return jnp.clip(jax.random.normal(jax.random.fold_in(key, 11), (TOKENS, KVH, HD), jnp.float32), -4.5, 4.5)


def draw_key_rows(key, part):
    return shared_keys(key).astype(jnp.bfloat16)


def draw_queries(key, part):
    base = jnp.clip(jax.random.normal(jax.random.fold_in(key, 12), (TOKENS, H, HD), jnp.float32), -4.5, 4.5)
    return base.astype(jnp.bfloat16)


def draw_windows(key, part):
    spread = jax.random.randint(jax.random.fold_in(key, 21), (H,), WINDOW // 2, WINDOW + 1)
    chosen = jax.random.randint(jax.random.fold_in(key, 22), (), 0, H)
    return jnp.where(jnp.arange(H) == chosen, WINDOW, spread).astype(jnp.int32)


def draw_sink_counts(key, part):
    spread = jax.random.randint(jax.random.fold_in(key, 31), (H,), 1, SINKS + 1)
    chosen = jax.random.randint(jax.random.fold_in(key, 32), (), 0, H)
    return jnp.where(jnp.arange(H) == chosen, SINKS, spread).astype(jnp.int32)


def steps_of(stream_key, dims, split, least, high):
    def one(dim, blocks):
        draws = jax.random.uniform(jax.random.fold_in(jax.random.fold_in(stream_key, 6), dim), (blocks,), jnp.float32, least / len(split), high / len(split))
        return jnp.repeat(jnp.exp(draws), dims[dim] // blocks).reshape((-1,) + (1,) * (len(dims) - dim - 1))

    level = one(*split[0])
    for cut in split[1:]:
        level = level * one(*cut)
    return level


def noise(own_key, extent, scale, most, pieces=(), held_as=jnp.bfloat16):
    values = jax.random.normal(own_key, extent, jnp.float32) * scale
    if len(pieces) > 0:
        values = steps_of(own_key, extent, pieces, -0.22, 0.18) * values
    return jnp.clip(values, min=-most, max=most).astype(held_as)


def setup_inputs(seed: int = 0) -> dict:
    streams_of = jax.random.split(jax.random.key(seed), 8)
    return {
        "queries": draw_queries(jax.random.fold_in(streams_of[7], 71), 0),
        "key_rows": draw_key_rows(jax.random.fold_in(streams_of[7], 71), 0),
        "value_rows": noise(streams_of[2], (TOKENS, KVH, HD), 4.0, 24.0, ((0, 64), (1, 8))),
        "windows": draw_windows(jax.random.fold_in(streams_of[7], 71), 0),
        "sink_counts": draw_sink_counts(jax.random.fold_in(streams_of[7], 71), 0),
        "sink_bias": jnp.clip(3.0 + 4.0 * jax.random.uniform(streams_of[5], (H,), jnp.float32) ** steps_of(streams_of[5], (H,), ((0, 8),), -0.2, 0.2), 3.0, 7.0),
        "out_weight": noise(streams_of[6], (H * HD, D), (H * HD) ** -0.5, 0.09375, ((0, 8),)),
    }


def attend_block(query_block, band_rows, sink_rows, first_pos, windows, sink_counts, sink_bias):
    tok_rows, local_heads, head_width = query_block.shape
    kv_local = band_rows.shape[2]
    group_size = local_heads // kv_local
    band_span = band_rows.shape[1]
    all_keys = jnp.concatenate([sink_rows[0], band_rows[0]], axis=0)
    all_values = jnp.concatenate([sink_rows[1], band_rows[1]], axis=0)
    grouped = query_block.reshape(tok_rows, kv_local, group_size, head_width)
    score_scale = 1.0 / (head_width ** 0.5)
    scores = jnp.einsum("tkgd,skd->kgts", grouped.astype(jnp.float32), all_keys.astype(jnp.float32)) * score_scale
    query_pos = first_pos + jnp.arange(tok_rows, dtype=jnp.int32)
    band_pos = first_pos + tok_rows - band_span + jnp.arange(band_span, dtype=jnp.int32)
    sink_pos = jnp.arange(SINKS, dtype=jnp.int32)
    key_pos = jnp.concatenate([sink_pos, band_pos])
    is_sink = jnp.concatenate([jnp.ones((SINKS,), bool), jnp.zeros((band_span,), bool)])
    head_window = windows.reshape(kv_local, group_size, 1, 1)
    head_sinks = sink_counts.reshape(kv_local, group_size, 1, 1)
    head_bias = sink_bias.reshape(kv_local, group_size, 1, 1)
    distance = query_pos[:, None] - key_pos[None, :]
    visible = (distance >= 0) & jnp.where(is_sink, key_pos < head_sinks, (distance < head_window) & (key_pos >= head_sinks))
    scores = scores + jnp.where(is_sink, head_bias, 0.0)
    masked = jnp.where(visible, scores, -1e30)
    highest = jnp.max(masked, axis=-1, keepdims=True)
    weights = jnp.where(visible, jnp.exp(masked - highest), 0.0)
    normed = (weights / jnp.sum(weights, axis=-1, keepdims=True)).astype(jnp.bfloat16)
    mixed = jnp.einsum("kgts,skd->tkgd", normed.astype(jnp.float32), all_values.astype(jnp.float32))
    return mixed.astype(jnp.bfloat16).reshape(tok_rows, local_heads * head_width)


def reference(queries, key_rows, value_rows, windows, sink_counts, sink_bias, out_weight):
    stacked = jnp.stack([key_rows, value_rows])
    padding = jnp.zeros((2, WINDOW, KVH, HD), jnp.bfloat16)
    padded = jnp.concatenate([padding, stacked], axis=1)
    sink_rows = stacked[:, :SINKS]

    def one_shard(shard_index):
        first_pos = (shard_index * TOK_DEV).astype(jnp.int32)
        query_block = lax.dynamic_slice_in_dim(queries, first_pos, TOK_DEV, 0)
        band_rows = lax.dynamic_slice_in_dim(padded, first_pos, TOK_DEV + WINDOW, 1)
        return attend_block(query_block, band_rows, sink_rows, first_pos, windows, sink_counts, sink_bias)

    attended = lax.map(one_shard, jnp.arange(N_SEQ, dtype=jnp.int32)).reshape(TOKENS, H * HD)
    group_rows = H * HD // N_HEAD
    total = jnp.zeros((TOKENS, D), jnp.float32)
    for member in range(N_HEAD):
        lower = member * group_rows
        term = jnp.dot(attended[:, lower:lower + group_rows], out_weight[lower:lower + group_rows], preferred_element_type=jnp.float32)
        total = total + lax.optimization_barrier(term.astype(jnp.bfloat16)).astype(jnp.float32)
    return total.astype(jnp.bfloat16)
```

```python
import jax
import jax.numpy as jnp
from jax import lax
from jax.experimental import pallas as pl
from jax.experimental.pallas import tpu as pltpu
from jax.sharding import PartitionSpec as P

TOK = 192
HEADS = 4
HD = 128
ROWS = TOK * HEADS
HALF = ROWS // 2
OUT_TOK = 24
D = 4096
NC = 4
CN = D // NC
KW = HEADS * HD
SINK_PAD = 16
LANES = 256
NEG = -1e30
LOG2E = 1.4426950408889634
MESH = pl.DeviceIdType.MESH
BF = jnp.bfloat16
F32 = jnp.float32


def remote(src, dst, send, recv, seq, head):
    return pltpu.make_async_remote_copy(
        src_ref=src, dst_ref=dst, send_sem=send, recv_sem=recv,
        device_id=(seq, head), device_id_type=MESH,
    )


def kernel(win_ref, cnt_ref, bias_ref, q_ref, k_ref, v_ref, w_ref, o_ref,
           kv, sink, q_in, q_f, q_f2, qs, w_own, w_oth, acc, m_st, l_st, a_buf, a_oth, pacc,
           sbuf, rbuf, relay,
           in_sem, x_send, y_send, kv_recv, s_send, s_recv, w_send, w_recv, a_send, a_recv,
           z_send, z_recv, relay_recv):
    seq = lax.axis_index("seq")
    head = lax.axis_index("head")
    row, y = seq // 8, seq % 8
    zl, core = head // 2, head % 2
    partner = head + 1 - 2 * core

    kv_in = [
        pltpu.make_async_copy(k_ref, kv.at[0, 0], in_sem.at[0]),
        pltpu.make_async_copy(v_ref, kv.at[0, 1], in_sem.at[1]),
    ]
    q_copy = pltpu.make_async_copy(q_ref, q_in, in_sem.at[2])
    w_copy = pltpu.make_async_copy(w_ref, w_own, in_sem.at[3])
    for copy in kv_in:
        copy.start()
    q_copy.start()
    w_copy.start()

    barrier = pltpu.get_barrier_semaphore()

    def greet(s, h):
        pl.semaphore_signal(barrier, inc=1, device_id=(s, h), device_id_type=MESH)

    @pl.when(row < 7)
    def _():
        greet(seq + 8, head)

    @pl.when(row > 0)
    def _():
        greet(seq - 8, head)

    for d in range(1, 8):
        greet(row * 8 + (y + d) % 8, head)
    greet(seq, partner)
    for d in range(1, 4):
        greet(seq, ((zl + d) % 4) * 2 + core)

    first = (row == 0) & (y == 0)
    later_first = (row > 0) & (y == 0)

    @pl.when(first)
    def _():
        for r in range(1, 8):
            greet(r * 8, head)

    @pl.when(later_first)
    def _():
        greet(0, head)

    expect = 11 + jnp.where(row < 7, 1, 0) + jnp.where(row > 0, 1, 0)
    expect = expect + jnp.where(first, 7, 0) + jnp.where(later_first, 1, 0)
    pl.semaphore_wait(barrier, expect)

    for copy in kv_in:
        copy.wait()

    def x_hop(part):
        return remote(kv.at[0, part], kv.at[8, part], x_send.at[part], kv_recv.at[8, part], seq + 8, head)

    def y_hop(source, d, part):
        return remote(kv.at[source, part], kv.at[d, part], y_send.at[d, part], kv_recv.at[d, part],
                      row * 8 + (y + d) % 8, head)

    order = (4, 3, 5, 2, 6, 1, 7)

    @pl.when(row < 7)
    def _():
        for part in range(2):
            x_hop(part).start()

    for d in order:
        @pl.when(y + d < 8)
        def _(d=d):
            for part in range(2):
                y_hop(0, d, part).start()

    sink_src = kv.at[0, :, pl.ds(0, SINK_PAD), :]

    def sink_row(r):
        return remote(sink_src, sink, s_send.at[r], s_recv, r * 8, head)

    def sink_y(src, d):
        return remote(src, sink, s_send.at[7 + d], s_recv, row * 8 + d, head)

    @pl.when(first)
    def _():
        for r in range(1, 8):
            sink_row(r).start()
        for d in range(1, 8):
            sink_y(sink_src, d).start()

    w_hop = remote(w_ref, w_oth, w_send, w_recv, seq, partner)
    w_hop.start()

    q_copy.wait()
    q_f[...] = q_in[...].astype(F32)
    for p in range(2):
        for h in range(HEADS):
            for d in range(4):
                q_f2[pl.ds(p * HALF + h * 96 + d * OUT_TOK, OUT_TOK), :] = q_f[
                    pl.ds((2 * d + p) * OUT_TOK * HEADS + h, OUT_TOK, HEADS), :]
    qs[...] = q_f2[...].astype(BF)

    m_st[...] = jnp.full_like(m_st, NEG)
    l_st[...] = jnp.zeros_like(l_st)
    acc[...] = jnp.zeros_like(acc)
    scale2 = LOG2E / HD ** 0.5

    def column_facts(tile):
        col = tile * LANES + lax.broadcasted_iota(jnp.int32, (1, LANES), 1)
        p = col // HALF
        h = (col % HALF) // 96
        token = (2 * ((col % 96) // OUT_TOK) + p) * OUT_TOK + col % OUT_TOK

        def per_head(ref):
            value = jnp.where(h == 0, ref[0], ref[1])
            value = jnp.where(h == 2, ref[2], value)
            return jnp.where(h == 3, ref[3], value)

        return seq * TOK + token, per_head

    def fold(tile, scores, values):
        lanes = pl.ds(tile * LANES, LANES)
        m_old = m_st[:, lanes]
        m_new = jnp.maximum(m_old, jnp.max(scores, axis=0, keepdims=True))
        weights = jnp.exp2(scores - m_new)
        alpha = jnp.exp2(m_old - m_new)
        m_st[:, lanes] = m_new
        l_st[:, lanes] = l_st[:, lanes] * alpha + jnp.sum(weights, axis=0, keepdims=True)
        mixed = lax.dot_general(values, weights.astype(BF), (((0,), (0,)), ((), ())),
                                preferred_element_type=F32)
        acc[:, lanes] = acc[:, lanes] * alpha + mixed

    def score_tile(tile, keys):
        return lax.dot_general(keys, qs[pl.ds(tile * LANES, LANES), :], (((1,), (1,)), ((), ())),
                               preferred_element_type=F32) * scale2

    def attend(slot):
        keys, values = kv[slot, 0], kv[slot, 1]
        for tile in range(ROWS // LANES):
            pos, per_head = column_facts(tile)
            key_pos = (seq - slot) * TOK + lax.broadcasted_iota(jnp.int32, (TOK, LANES), 0)
            distance = pos - key_pos
            visible = (distance >= 0) & (distance < per_head(win_ref)) & (key_pos >= per_head(cnt_ref))
            fold(tile, jnp.where(visible, score_tile(tile, keys), NEG), values)

    def attend_sinks():
        keys, values = sink[0], sink[1]
        for tile in range(ROWS // LANES):
            pos, per_head = column_facts(tile)
            key_pos = lax.broadcasted_iota(jnp.int32, (SINK_PAD, LANES), 0)
            visible = (pos >= key_pos) & (key_pos < per_head(cnt_ref))
            scores = score_tile(tile, keys) + per_head(bias_ref) * LOG2E
            fold(tile, jnp.where(visible, scores, NEG), values)

    @pl.when(first)
    def _():
        sink[...] = kv[0, :, :SINK_PAD, :]

    def sink_arrival():
        return remote(sink, sink, s_send.at[0], s_recv, seq, partner)

    def kv_arrival(slot, part):
        return remote(kv.at[slot, part], kv.at[slot, part], y_send.at[0, part], kv_recv.at[slot, part], seq, partner)

    @pl.when(row > 0)
    def _():
        for part in range(2):
            kv_arrival(8, part).wait_recv()
            for d in order:
                @pl.when(y + d >= 8)
                def _(d=d, part=part):
                    y_hop(8, d, part).start()

    @pl.when(jnp.logical_not(first))
    def _():
        sink_arrival().wait_recv()

    @pl.when(later_first)
    def _():
        for d in range(1, 8):
            sink_y(sink, d).start()

    def step(slot, carry):
        @pl.when(seq >= slot)
        def _():
            @pl.when((slot > 0) & (slot < 8))
            def _():
                for part in range(2):
                    kv_arrival(slot, part).wait_recv()

            attend(slot)

        return carry

    lax.fori_loop(0, 9, step, 0)
    attend_sinks()

    for tile in range(ROWS // 128):
        lanes = pl.ds(tile * 128, 128)
        done = acc[:, lanes] / l_st[:, lanes]
        a_buf[lanes, :] = done.T.astype(BF)

    mine = pl.multiple_of(core * HALF, HALF)
    theirs = pl.multiple_of(HALF - core * HALF, HALF)
    a_hop = remote(a_buf.at[pl.ds(theirs, HALF), :], a_oth, a_send, a_recv, seq, partner)
    a_hop.start()

    a_mine = jnp.concatenate(
        [a_buf[pl.ds(pl.multiple_of(mine + h * 96, 96), 96), :] for h in range(HEADS)], axis=1)
    w_copy.wait()

    for j in range(NC):
        cols = pl.ds(j * CN, CN)
        pacc[:, cols] = jnp.dot(a_mine, w_own[:, cols], preferred_element_type=F32)
    a_hop.wait_recv()
    w_hop.wait_recv()
    a_other = jnp.concatenate([a_oth[pl.ds(h * 96, 96), :] for h in range(HEADS)], axis=1)

    is_end = (zl == 0) | (zl == 3)
    is_mid = jnp.logical_not(is_end)
    n1 = 1 + zl // 3
    n2 = 3 - n1
    n3 = 3 - zl
    e1 = (zl - 1) * 3
    m2 = 3 - zl
    e2 = 3 - e1

    def item(d, j):
        return pacc[pl.ds(pl.multiple_of(d * OUT_TOK, 8), OUT_TOK), pl.ds(j * CN, CN)]

    def z_hop(n, j, to):
        return remote(sbuf.at[n, j], rbuf.at[zl, j], z_send.at[n, j], z_recv.at[zl, j], seq, to * 2 + core)

    def relay_hop(j):
        return remote(sbuf.at[2, j], relay.at[j], z_send.at[2, j], relay_recv.at[j], seq, n1 * 2 + core)

    def relay_arrival(j):
        return remote(relay.at[j], relay.at[j], z_send.at[2, j], relay_recv.at[j], seq, partner)

    def z_arrival(source, j):
        return remote(rbuf.at[source, j], rbuf.at[source, j], z_send.at[0, j], z_recv.at[source, j], seq, partner)

    for j in range(NC):
        cols = pl.ds(j * CN, CN)
        pacc[:, cols] += jnp.dot(a_other, w_oth[:, cols], preferred_element_type=F32)

        @pl.when(is_end)
        def _(j=j):
            sbuf[2, j] = item(n3, j).astype(BF)
            relay_hop(j).start()

        @pl.when(is_mid)
        def _(j=j):
            sbuf[0, j] = item(m2, j).astype(BF)
            z_hop(0, j, m2).start()
            sbuf[1, j] = item(e1, j).astype(BF)
            z_hop(1, j, e1).start()

    @pl.when(is_end)
    def _():
        for n, to in ((0, n2), (1, n1)):
            for j in range(NC):
                sbuf[n, j] = item(to, j).astype(BF)
                z_hop(n, j, to).start()

    @pl.when(is_mid)
    def _():
        for j in range(NC):
            relay_arrival(j).wait_recv()
            sbuf[2, j] = (item(e2, j) + relay[j].astype(F32)).astype(BF)
            z_hop(2, j, e2).start()

    def collect(sources):
        for j in range(NC):
            total = item(zl, j)
            for source in sources:
                z_arrival(source, j).wait_recv()
                total = total + rbuf[source, j].astype(F32)
            o_ref[:, pl.ds(j * CN, CN)] = total.astype(BF)

    @pl.when(is_end)
    def _():
        collect((n1, n2))

    @pl.when(is_mid)
    def _():
        collect((m2, e1, e2))

    @pl.when(row < 7)
    def _():
        for part in range(2):
            x_hop(part).wait_send()

    for d in order:
        @pl.when((y + d < 8) | (row > 0))
        def _(d=d):
            for part in range(2):
                y_hop(0, d, part).wait_send()

    @pl.when(first)
    def _():
        for r in range(1, 8):
            sink_row(r).wait_send()

    @pl.when(y == 0)
    def _():
        for d in range(1, 8):
            sink_y(sink, d).wait_send()

    w_hop.wait_send()
    a_hop.wait_send()
    for j in range(NC):
        for n in range(3):
            z_hop(n, j, zl).wait_send()


def shards(queries, key_rows, value_rows, windows, sink_counts, sink_bias, out_weight):
    smem = pl.BlockSpec(memory_space=pltpu.SMEM)
    hbm = pl.BlockSpec(memory_space=pl.ANY)
    return pl.pallas_call(
        kernel,
        out_shape=jax.ShapeDtypeStruct((OUT_TOK, D), BF),
        in_specs=[smem] * 3 + [hbm] * 4,
        out_specs=pl.BlockSpec(memory_space=pltpu.VMEM),
        scratch_shapes=[
            pltpu.VMEM((9, 2, TOK, HD), BF),
            pltpu.VMEM((2, SINK_PAD, HD), BF),
            pltpu.VMEM((ROWS, HD), BF),
            pltpu.VMEM((ROWS, HD), F32),
            pltpu.VMEM((ROWS, HD), F32),
            pltpu.VMEM((ROWS, HD), BF),
            pltpu.VMEM((KW, D), BF),
            pltpu.VMEM((KW, D), BF),
            pltpu.VMEM((HD, ROWS), F32),
            pltpu.VMEM((1, ROWS), F32),
            pltpu.VMEM((1, ROWS), F32),
            pltpu.VMEM((ROWS, HD), BF),
            pltpu.VMEM((HALF, HD), BF),
            pltpu.VMEM((96, D), F32),
            pltpu.VMEM((3, NC, OUT_TOK, CN), BF),
            pltpu.VMEM((4, NC, OUT_TOK, CN), BF),
            pltpu.VMEM((NC, OUT_TOK, CN), BF),
            pltpu.SemaphoreType.DMA((4,)),
            pltpu.SemaphoreType.DMA((2,)),
            pltpu.SemaphoreType.DMA((8, 2)),
            pltpu.SemaphoreType.DMA((9, 2)),
            pltpu.SemaphoreType.DMA((15,)),
            pltpu.SemaphoreType.DMA,
            pltpu.SemaphoreType.DMA,
            pltpu.SemaphoreType.DMA,
            pltpu.SemaphoreType.DMA,
            pltpu.SemaphoreType.DMA,
            pltpu.SemaphoreType.DMA((3, NC)),
            pltpu.SemaphoreType.DMA((4, NC)),
            pltpu.SemaphoreType.DMA((NC,)),
        ],
        compiler_params=pltpu.CompilerParams(
            collective_id=0, has_side_effects=True, vmem_limit_bytes=40 * 1024 * 1024),
    )(windows, sink_counts, sink_bias, queries.reshape(ROWS, HD), key_rows.reshape(TOK, HD),
      value_rows.reshape(TOK, HD), out_weight)


def solution(mesh):
    return jax.shard_map(
        shards,
        mesh=mesh,
        in_specs=(
            P("seq", "head", None),
            P("seq", "head", None),
            P("seq", "head", None),
            P("head"),
            P("head"),
            P("head"),
            P("head", None),
        ),
        out_specs=P(("seq", "head"), None),
        check_vma=False,
    )
```

```python
import jax
import jax.numpy as jnp
from jax import lax
from jax.experimental import pallas as pl
from jax.experimental.pallas import tpu as pltpu
from jax.sharding import PartitionSpec as P

TOK = 192
HEADS = 4
HD = 128
ROWS = TOK * HEADS
HALF = ROWS // 2
OUT_TOK = 24
D = 4096
NC = 4
CN = D // NC
KW = HEADS * HD
SINK_PAD = 16
PARTS = 4
PART_ROWS = 2 * TOK // PARTS
LANES = 256
NEG = -1e30
LOG2E = 1.4426950408889634
MESH = pl.DeviceIdType.MESH
BF = jnp.bfloat16
F32 = jnp.float32


USUAL = (
    (8, 1, 2, 7, 6, 5, 3, 4),
    (1, 8, 7, 6, 2, 5, 3, 4),
    (1, 8, 2, 7, 6, 5, 3, 4),
    (1, 8, 2, 7, 3, 6, 5, 4),
    (1, 8, 2, 7, 3, 6, 5, 4),
    (1, 8, 7, 2, 6, 3, 5, 4),
    (8, 7, 2, 6, 1, 5, 3, 4),
    (8, 7, 6, 1, 3, 5, 2, 4),
)
CROSSED = (
    (8, 1, 7, 2, 6, 5, 3, 4),
    (1, 8, 7, 6, 2, 5, 3, 4),
    (1, 2, 8, 7, 6, 5, 3, 4),
    (1, 2, 8, 3, 7, 6, 5, 4),
    (1, 2, 8, 7, 3, 6, 4, 5),
    (1, 2, 8, 7, 3, 6, 4, 5),
    (1, 2, 8, 7, 3, 6, 5, 4),
    (1, 7, 8, 3, 6, 5, 2, 4),
)
TOP = (
    (8, 1, 2, 3, 4, 5, 6, 7),
    (8, 1, 2, 3, 4, 5, 6, 7),
    (8, 1, 2, 3, 4, 5, 6, 7),
    (8, 1, 2, 3, 4, 5, 6, 7),
    (8, 1, 2, 3, 4, 5, 6, 7),
    (8, 1, 2, 3, 5, 4, 6, 7),
    (8, 1, 2, 6, 3, 5, 4, 7),
    (8, 7, 1, 6, 3, 5, 2, 4),
)


def packed(order):
    return sum((slot - 1) << (3 * k) for k, slot in enumerate(order))


def remote(src, dst, send, recv, seq, head):
    return pltpu.make_async_remote_copy(
        src_ref=src, dst_ref=dst, send_sem=send, recv_sem=recv,
        device_id=(seq, head), device_id_type=MESH,
    )


def kernel(win_in, cnt_in, bias_in, q_ref, k_ref, v_ref, w_ref, o_ref,
           win_ref, cnt_ref, bias_ref, kv, sink, q_in, q_f, q_f2, qs, w_own, w_oth, acc, m_st, l_st, a_buf, a_oth, pacc,
           sbuf, rbuf, relay,
           in_sem, x_send, y_send, far_send, kv_recv, s_send, s_recv, w_send, w_recv, a_send, a_recv,
           z_send, z_recv, relay_recv):
    seq = lax.axis_index("seq")
    head = lax.axis_index("head")
    row, y = seq // 8, seq % 8
    zl, core = head // 2, head % 2
    partner = head + 1 - 2 * core

    half = TOK // PART_ROWS
    kv_in = [
        pltpu.make_async_copy(
            ref.at[pl.ds(i * PART_ROWS, PART_ROWS), :], kv.at[0, base + i], in_sem.at[base + i])
        for base, ref in ((0, k_ref), (half, v_ref))
        for i in range(half)
    ]
    later_in = [
        pltpu.make_async_copy(q_ref, q_in, in_sem.at[PARTS]),
        pltpu.make_async_copy(win_in, win_ref, in_sem.at[PARTS + 2]),
        pltpu.make_async_copy(cnt_in, cnt_ref, in_sem.at[PARTS + 3]),
        pltpu.make_async_copy(bias_in, bias_ref, in_sem.at[PARTS + 4]),
    ]
    w_copy = pltpu.make_async_copy(w_ref, w_own, in_sem.at[PARTS + 1])
    for copy in kv_in + later_in:
        copy.start()
    w_copy.start()

    is_end = (zl == 0) | (zl == 3)
    is_mid = jnp.logical_not(is_end)
    n1 = 1 + zl // 3
    n2 = 3 - n1
    n3 = 3 - zl
    e1 = (zl - 1) * 3
    m2 = 3 - zl
    e2 = 3 - e1
    first = (row == 0) & (y == 0)
    inner = row > 0

    barrier = pltpu.get_barrier_semaphore()

    def greet(s, h, when=None):
        def signal():
            pl.semaphore_signal(barrier, inc=1, device_id=(s, h), device_id_type=MESH)

        if when is None:
            signal()
        else:
            pl.when(when)(signal)

    greet(seq - 1, head, y >= 1)
    greet(seq + 1, head, (y <= 6) & (inner | (y >= 5)))
    for d in (5, 6, 7):
        greet(seq + d, head, (y == 0) & inner)
    for d in (7, 6, 5):
        greet(seq - d, head, y == 7)
    greet(jnp.where(row == 0, seq + 24, jnp.where(row == 4, seq - 32, seq - 8)), head)
    greet(seq - 24, head, (row == 3) | (row == 7))
    greet(row * 8, head, (row == 0) & (y >= 1))
    greet(seq, partner)
    greet(seq, n1 * 2 + core, is_end)
    greet(seq, n2 * 2 + core, is_end)
    for d in range(1, 4):
        greet(seq, ((zl + d) % 4) * 2 + core, is_mid)

    def count(flag):
        return jnp.where(flag, 1, 0)

    expect = 3 + count(is_mid) + count(y < 7) + count((y >= 1) & (inner | (y >= 6)))
    expect = expect + count((y >= 5) & inner) + count(y <= 2) + count(row < 7) + count(row == 4)
    expect = expect + jnp.where(row == 0, 2, 0) + jnp.where(first, 7, 0)
    with jax.named_scope("greet"):
        pl.semaphore_wait(barrier, expect)

    for copy in kv_in:
        copy.wait()

    def own_hop(part):
        return remote(kv.at[0, part], kv.at[1, part], y_send.at[0, part], kv_recv.at[1, part], seq + 1, head)

    def far_hop(source, column, part):
        slot = jnp.where(column == 7, 7 - y, 8 - y)
        return remote(kv.at[source, part], kv.at[slot, part], far_send.at[part], kv_recv.at[slot, part],
                      row * 8 + column, head)

    def x_hop(part):
        return remote(kv.at[0, part], kv.at[8, part], x_send.at[part], kv_recv.at[8, part],
                      jnp.where(row == 3, seq - 24, seq + 8), head)

    crossing = row == 0

    def relay_of(slot):
        own = jnp.where((slot <= 3) & (y <= 6), 1, jnp.where(slot >= 6, -1, 0))
        before = jnp.where((slot >= 5) & (y >= 1), -1, jnp.where(slot <= 2, 1, 0))
        return jnp.where(slot <= y, own, before)

    def relay_hop(slot, part):
        turn = relay_of(slot)
        across = crossing & (slot == 8)
        to = jnp.where(across, seq + 32, row * 8 + (y + turn + 8) % 8)
        land = jnp.where(across, 8, slot + turn)
        return remote(kv.at[slot, part], kv.at[land, part], y_send.at[slot, part], kv_recv.at[land, part],
                      to, head)

    def held(slot):
        return (slot <= y) | inner | (slot == 8)

    def relays(slot):
        return (relay_of(slot) != 0) | (crossing & (slot == 8))

    sink_src = kv.at[0, 0, pl.ds(0, SINK_PAD), :]
    sink_src_v = kv.at[0, half, pl.ds(0, SINK_PAD), :]

    def sink_hops(keys, values, n, to):
        return [
            remote(keys, sink.at[0], s_send.at[n, 0], s_recv.at[0], to, head),
            remote(values, sink.at[1], s_send.at[n, 1], s_recv.at[1], to, head),
        ]

    forwards = (
        (0, 8, (row == 0) | (row == 1) | (row == 4) | (row == 5)),
        (1, 24, (row == 0) | (row == 4)),
        (2, 32, row == 0),
    )

    def pass_sinks(keys, values):
        for n, offset, flag in forwards:
            @pl.when(flag)
            def _(n=n, offset=offset):
                for copy in sink_hops(keys, values, n, seq + offset):
                    copy.start()

    @pl.when(first)
    def _():
        for d in range(1, 8):
            for copy in sink_hops(sink_src, sink_src_v, 2 + d, d):
                copy.start()
        pass_sinks(sink_src, sink_src_v)

    @pl.when(row < 7)
    def _():
        for part in range(PARTS):
            x_hop(part).start()

    @pl.when(y < 7)
    def _():
        for part in range(PARTS):
            own_hop(part).start()

    @pl.when(y <= 2)
    def _():
        for part in range(PARTS):
            far_hop(0, 7, part).start()

    w_hop = remote(w_ref, w_oth, w_send, w_recv, seq, partner)
    w_hop.start()

    for copy in later_in:
        copy.wait()
    q_f[...] = q_in[...].astype(F32)
    for p in range(2):
        for h in range(HEADS):
            for d in range(4):
                q_f2[pl.ds(p * HALF + h * 96 + d * OUT_TOK, OUT_TOK), :] = q_f[
                    pl.ds((2 * d + p) * OUT_TOK * HEADS + h, OUT_TOK, HEADS), :]
    qs[...] = q_f2[...].astype(BF)

    m_st[...] = jnp.full_like(m_st, NEG)
    l_st[...] = jnp.zeros_like(l_st)
    acc[...] = jnp.zeros_like(acc)
    scale2 = LOG2E / HD ** 0.5

    def column_facts(tile):
        col = tile * LANES + lax.broadcasted_iota(jnp.int32, (1, LANES), 1)
        p = col // HALF
        h = (col % HALF) // 96
        token = (2 * ((col % 96) // OUT_TOK) + p) * OUT_TOK + col % OUT_TOK

        def per_head(ref):
            value = jnp.where(h == 0, ref[0], ref[1])
            value = jnp.where(h == 2, ref[2], value)
            return jnp.where(h == 3, ref[3], value)

        return seq * TOK + token, per_head

    def fold(tile, scores, values):
        lanes = pl.ds(tile * LANES, LANES)
        m_old = m_st[:, lanes]
        m_new = jnp.maximum(m_old, jnp.max(scores, axis=0, keepdims=True))
        weights = jnp.exp2(scores - m_new)
        alpha = jnp.exp2(m_old - m_new)
        m_st[:, lanes] = m_new
        l_st[:, lanes] = l_st[:, lanes] * alpha + jnp.sum(weights, axis=0, keepdims=True)
        mixed = lax.dot_general(values, weights.astype(BF), (((0,), (0,)), ((), ())),
                                preferred_element_type=F32)
        acc[:, lanes] = acc[:, lanes] * alpha + mixed

    def score_tile(tile, keys):
        return lax.dot_general(keys, qs[pl.ds(tile * LANES, LANES), :], (((1,), (1,)), ((), ())),
                               preferred_element_type=F32) * scale2

    def attend(slot):
        keys = kv[slot, :half].reshape(TOK, HD)
        values = kv[slot, half:].reshape(TOK, HD)
        for tile in range(ROWS // LANES):
            pos, per_head = column_facts(tile)
            key_pos = (seq - slot) * TOK + lax.broadcasted_iota(jnp.int32, (TOK, LANES), 0)
            distance = pos - key_pos
            visible = (distance >= 0) & (distance < per_head(win_ref)) & (key_pos >= per_head(cnt_ref))
            fold(tile, jnp.where(visible, score_tile(tile, keys), NEG), values)

    def attend_sinks():
        keys, values = sink[0], sink[1]
        for tile in range(ROWS // LANES):
            pos, per_head = column_facts(tile)
            key_pos = lax.broadcasted_iota(jnp.int32, (SINK_PAD, LANES), 0)
            visible = (pos >= key_pos) & (key_pos < per_head(cnt_ref))
            scores = score_tile(tile, keys) + per_head(bias_ref) * LOG2E
            fold(tile, jnp.where(visible, scores, NEG), values)

    @pl.when(first)
    def _():
        sink[0] = kv[0, 0, :SINK_PAD, :]
        sink[1] = kv[0, half, :SINK_PAD, :]

    def sink_arrival():
        with jax.named_scope("sink_wait"):
            for copy in sink_hops(sink.at[0], sink.at[1], 0, seq):
                copy.wait_recv()

    def kv_arrival(slot, part):
        return remote(kv.at[slot, part], kv.at[slot, part], far_send.at[part], kv_recv.at[slot, part],
                      seq, partner)

    word = jnp.int32(0)
    for column in range(8):
        chosen = jnp.where(row == 4, packed(CROSSED[column]), packed(USUAL[column]))
        chosen = jnp.where(row == 0, packed(TOP[column]), chosen)
        word = jnp.where(y == column, chosen, word)
    sink_step = jnp.where(row == 0, 1, jnp.where(row == 5, 6, 4))
    passes = (row == 0) | (row == 1) | (row == 4) | (row == 5)

    with jax.named_scope("attend"):
        attend(0)

    def step(k, carry):
        slot = (lax.shift_right_logical(word, 3 * k) & 7) + 1

        @pl.when((k == sink_step) & passes & jnp.logical_not(first))
        def _():
            sink_arrival()
            pass_sinks(sink.at[0], sink.at[1])

        @pl.when(held(slot))
        def _():
            for part in range(PARTS):
                with jax.named_scope("kv_wait"):
                    kv_arrival(slot, part).wait_recv()

                @pl.when(relays(slot))
                def _(part=part):
                    relay_hop(slot, part).start()

                @pl.when((slot == 8) & (y >= 5) & inner)
                def _(part=part):
                    far_hop(8, 0, part).start()

        @pl.when(seq >= slot)
        def _():
            with jax.named_scope("attend"):
                attend(slot)

        return carry

    lax.fori_loop(0, 8, step, 0)

    @pl.when(jnp.logical_not(passes))
    def _():
        sink_arrival()

    attend_sinks()

    for tile in range(ROWS // 128):
        lanes = pl.ds(tile * 128, 128)
        done = acc[:, lanes] / l_st[:, lanes]
        a_buf[lanes, :] = done.T.astype(BF)

    mine = pl.multiple_of(core * HALF, HALF)
    theirs = pl.multiple_of(HALF - core * HALF, HALF)
    a_hop = remote(a_buf.at[pl.ds(theirs, HALF), :], a_oth, a_send, a_recv, seq, partner)
    a_hop.start()

    a_mine = jnp.concatenate(
        [a_buf[pl.ds(pl.multiple_of(mine + h * 96, 96), 96), :] for h in range(HEADS)], axis=1)
    w_copy.wait()

    for j in range(NC):
        cols = pl.ds(j * CN, CN)
        pacc[:, cols] = jnp.dot(a_mine, w_own[:, cols], preferred_element_type=F32)
    with jax.named_scope('a_wait'):
        a_hop.wait_recv()
    with jax.named_scope('w_wait'):
        w_hop.wait_recv()
    a_other = jnp.concatenate([a_oth[pl.ds(h * 96, 96), :] for h in range(HEADS)], axis=1)

    def item(d, j):
        return pacc[pl.ds(pl.multiple_of(d * OUT_TOK, 8), OUT_TOK), pl.ds(j * CN, CN)]

    def z_hop(n, j, to):
        return remote(sbuf.at[n, j], rbuf.at[zl, j], z_send.at[n, j], z_recv.at[zl, j], seq, to * 2 + core)

    def line_hop(j):
        return remote(sbuf.at[2, j], relay.at[j], z_send.at[2, j], relay_recv.at[j], seq, n1 * 2 + core)

    def relay_arrival(j):
        return remote(relay.at[j], relay.at[j], z_send.at[2, j], relay_recv.at[j], seq, partner)

    def z_arrival(source, j):
        return remote(rbuf.at[source, j], rbuf.at[source, j], z_send.at[0, j], z_recv.at[source, j], seq, partner)

    for j in range(NC):
        cols = pl.ds(j * CN, CN)
        pacc[:, cols] += jnp.dot(a_other, w_oth[:, cols], preferred_element_type=F32)

        @pl.when(is_end)
        def _(j=j):
            sbuf[2, j] = item(n3, j).astype(BF)
            line_hop(j).start()

        @pl.when(is_mid)
        def _(j=j):
            sbuf[0, j] = item(m2, j).astype(BF)
            z_hop(0, j, m2).start()
            sbuf[1, j] = item(e1, j).astype(BF)
            z_hop(1, j, e1).start()

    @pl.when(is_end)
    def _():
        for n, to in ((0, n2), (1, n1)):
            for j in range(NC):
                sbuf[n, j] = item(to, j).astype(BF)
                z_hop(n, j, to).start()

    @pl.when(is_mid)
    def _():
        for j in range(NC):
            with jax.named_scope('relay_wait'):
                relay_arrival(j).wait_recv()
            sbuf[2, j] = (item(e2, j) + relay[j].astype(F32)).astype(BF)
            z_hop(2, j, e2).start()

    def collect(sources):
        for j in range(NC):
            total = item(zl, j)
            for source in sources:
                with jax.named_scope('z_wait'):
                    z_arrival(source, j).wait_recv()
                total = total + rbuf[source, j].astype(F32)
            o_ref[:, pl.ds(j * CN, CN)] = total.astype(BF)

    @pl.when(is_end)
    def _():
        collect((n1, n2))

    @pl.when(is_mid)
    def _():
        collect((m2, e1, e2))

    @pl.when(row < 7)
    def _():
        for part in range(PARTS):
            x_hop(part).wait_send()

    @pl.when(y < 7)
    def _():
        for part in range(PARTS):
            own_hop(part).wait_send()

    @pl.when((y <= 2) | ((y >= 5) & inner))
    def _():
        for part in range(PARTS):
            far_hop(0, 7, part).wait_send()

    def drain(slot, carry):
        @pl.when(held(slot) & relays(slot))
        def _():
            for part in range(PARTS):
                relay_hop(slot, part).wait_send()

        return carry

    lax.fori_loop(1, 9, drain, 0)

    for n, offset, flag in forwards:
        @pl.when(flag)
        def _(n=n, offset=offset):
            for copy in sink_hops(sink.at[0], sink.at[1], n, seq + offset):
                copy.wait_send()

    @pl.when(first)
    def _():
        for d in range(1, 8):
            for copy in sink_hops(sink.at[0], sink.at[1], 2 + d, d):
                copy.wait_send()

    w_hop.wait_send()
    a_hop.wait_send()
    for j in range(NC):
        for n in range(3):
            z_hop(n, j, zl).wait_send()


def shards(queries, key_rows, value_rows, windows, sink_counts, sink_bias, out_weight):
    hbm = pl.BlockSpec(memory_space=pltpu.HBM)
    return pl.pallas_call(
        kernel,
        out_shape=pltpu.VMEM((OUT_TOK, D), BF),
        in_specs=[hbm] * 7,
        out_specs=pl.BlockSpec(memory_space=pltpu.VMEM),
        scratch_shapes=[
            pltpu.SMEM((HEADS,), jnp.int32),
            pltpu.SMEM((HEADS,), jnp.int32),
            pltpu.SMEM((HEADS,), F32),
            pltpu.VMEM((9, PARTS, PART_ROWS, HD), BF),
            pltpu.VMEM((2, SINK_PAD, HD), BF),
            pltpu.VMEM((ROWS, HD), BF),
            pltpu.VMEM((ROWS, HD), F32),
            pltpu.VMEM((ROWS, HD), F32),
            pltpu.VMEM((ROWS, HD), BF),
            pltpu.VMEM((KW, D), BF),
            pltpu.VMEM((KW, D), BF),
            pltpu.VMEM((HD, ROWS), F32),
            pltpu.VMEM((1, ROWS), F32),
            pltpu.VMEM((1, ROWS), F32),
            pltpu.VMEM((ROWS, HD), BF),
            pltpu.VMEM((HALF, HD), BF),
            pltpu.VMEM((96, D), F32),
            pltpu.VMEM((3, NC, OUT_TOK, CN), BF),
            pltpu.VMEM((4, NC, OUT_TOK, CN), BF),
            pltpu.VMEM((NC, OUT_TOK, CN), BF),
            pltpu.SemaphoreType.DMA((PARTS + 5,)),
            pltpu.SemaphoreType.DMA((PARTS,)),
            pltpu.SemaphoreType.DMA((9, PARTS)),
            pltpu.SemaphoreType.DMA((PARTS,)),
            pltpu.SemaphoreType.DMA((9, PARTS)),
            pltpu.SemaphoreType.DMA((10, 2)),
            pltpu.SemaphoreType.DMA((2,)),
            pltpu.SemaphoreType.DMA,
            pltpu.SemaphoreType.DMA,
            pltpu.SemaphoreType.DMA,
            pltpu.SemaphoreType.DMA,
            pltpu.SemaphoreType.DMA((3, NC)),
            pltpu.SemaphoreType.DMA((4, NC)),
            pltpu.SemaphoreType.DMA((NC,)),
        ],
        compiler_params=pltpu.CompilerParams(
            collective_id=0, has_side_effects=True, vmem_limit_bytes=67043328 - 512 * 1024),
    )(windows, sink_counts, sink_bias, queries.reshape(ROWS, HD), key_rows.reshape(TOK, HD),
      value_rows.reshape(TOK, HD), out_weight)


def solution(mesh):
    return jax.shard_map(
        shards,
        mesh=mesh,
        in_specs=(
            P("seq", "head", None),
            P("seq", "head", None),
            P("seq", "head", None),
            P("head"),
            P("head"),
            P("head"),
            P("head", None),
        ),
        out_specs=P(("seq", "head"), None),
        check_vma=False,
    )
```

```python
import jax
import jax.numpy as jnp
from jax import lax
from jax.experimental import pallas as pl
from jax.experimental.pallas import tpu as pltpu
from jax.sharding import PartitionSpec as P

TOK = 192
HEADS = 4
HD = 128
ROWS = TOK * HEADS
HALF = ROWS // 2
OUT_TOK = 24
D = 4096
NC = 4
CN = D // NC
KW = HEADS * HD
SINK_PAD = 16
PARTS = 4
PART_ROWS = 2 * TOK // PARTS
LANES = 256
NEG = -1e30
LOG2E = 1.4426950408889634
MESH = pl.DeviceIdType.MESH
BF = jnp.bfloat16
F32 = jnp.float32


USUAL = (
    (1, 2, 3, 8, 7, 6, 5, 4),
    (8, 1, 7, 6, 5, 3, 2, 4),
    (8, 7, 6, 3, 1, 2, 4, 5),
    (8, 1, 2, 6, 5, 7, 4, 3),
    (8, 1, 7, 2, 4, 6, 5, 3),
    (8, 1, 7, 2, 6, 5, 3, 4),
    (8, 7, 1, 6, 4, 2, 5, 3),
    (8, 7, 1, 5, 6, 2, 3, 4),
)
CROSSED = (
    (8, 1, 7, 2, 6, 5, 3, 4),
    (1, 8, 7, 6, 2, 5, 3, 4),
    (1, 2, 8, 7, 6, 5, 3, 4),
    (1, 2, 8, 3, 7, 6, 5, 4),
    (1, 2, 8, 7, 3, 6, 4, 5),
    (1, 2, 8, 7, 3, 6, 4, 5),
    (1, 2, 8, 7, 3, 6, 5, 4),
    (1, 7, 8, 3, 6, 5, 2, 4),
)
TOP = (
    (8, 1, 2, 3, 7, 6, 5, 4),
    (8, 1, 7, 6, 5, 3, 2, 4),
    (8, 1, 2, 7, 6, 3, 4, 5),
    (8, 1, 2, 3, 6, 5, 7, 4),
    (8, 1, 2, 4, 3, 7, 6, 5),
    (8, 1, 2, 5, 3, 4, 7, 6),
    (8, 1, 6, 4, 2, 5, 3, 7),
    (8, 7, 1, 5, 6, 2, 3, 4),
)
USUAL_PASS = (
    ((1, 7, 2), (2,), (1, 2), (1,), (), (), (), (), ()),
    ((3, 7), (4,), (), (), (), (0,), (0,), (0,), (0,)),
    ((3, 7), (), (), (3, 1), (), (), (1,), (1,), (1,)),
    ((4,), (4,), (5, 2, 4), (), (), (), (2,), (), (2,)),
    ((5, 6), (5,), (5,), (), (3,), (), (), (3,), (3, 2)),
    ((6,), (7,), (7, 6), (), (), (), (4,), (3, 4), (4, 0)),
    ((7,), (7,), (), (), (), (), (), (5,), (0, 5)),
    ((), (), (), (), (), (6,), (6,), (5, 6), (6, 0)),
)
CROSSED_PASS = (
    ((1, 7), (1,), (1,), (), (), (), (), (), ()),
    ((2, 7), (2,), (2,), (), (), (0,), (0,), (0,), (0,)),
    ((3, 7), (3,), (3,), (), (), (1,), (1,), (1,), (1,)),
    ((4,), (4,), (4,), (4,), (), (2,), (2,), (2,), (2,)),
    ((5,), (5,), (5,), (5,), (), (3,), (3,), (3,), (3,)),
    ((6,), (6,), (6,), (6,), (), (), (4,), (4,), (4, 0)),
    ((7,), (7,), (7,), (7,), (), (), (5,), (5,), (5, 0)),
    ((), (), (), (), (), (), (6,), (6,), (6, 0)),
)
FAN = 3


def packed(order):
    return sum((slot - 1) << (3 * k) for k, slot in enumerate(order))


def pass_word(table, y, i):
    word = 0
    for slot, columns in enumerate(table[y]):
        if i < len(columns):
            word |= ((columns[i] - y) % 8) << (3 * slot)
    return word


def peer_word(table, y, own_only):
    senders, receivers = set(), set()
    for column in range(8):
        for slot, columns in enumerate(table[column]):
            if own_only and slot > column:
                continue
            if column == y:
                receivers.update(columns)
            if y in columns:
                senders.add(column)
    mask = sum(1 << ((column - y) % 8) for column in senders)
    return mask + 256 * len(receivers)


def remote(src, dst, send, recv, seq, head):
    return pltpu.make_async_remote_copy(
        src_ref=src, dst_ref=dst, send_sem=send, recv_sem=recv,
        device_id=(seq, head), device_id_type=MESH,
    )


def kernel(win_in, cnt_in, bias_in, q_ref, k_ref, v_ref, w_ref, o_ref,
           win_ref, cnt_ref, bias_ref, kv, sink, q_in, q_f, q_f2, qs, w_own, w_oth, acc, m_st, l_st, a_buf, a_oth, pacc,
           sbuf, rbuf, relay,
           in_sem, x_send, y_send, kv_recv, s_send, s_recv, w_send, w_recv, a_send, a_recv,
           z_send, z_recv, relay_recv, ready):
    seq = lax.axis_index("seq")
    head = lax.axis_index("head")
    row, y = seq // 8, seq % 8
    zl, core = head // 2, head % 2
    partner = head + 1 - 2 * core

    half = TOK // PART_ROWS
    kv_in = [
        pltpu.make_async_copy(
            ref.at[pl.ds(i * PART_ROWS, PART_ROWS), :], kv.at[0, base + i], in_sem.at[base + i])
        for base, ref in ((0, k_ref), (half, v_ref))
        for i in range(half)
    ]
    later_in = [
        pltpu.make_async_copy(q_ref, q_in, in_sem.at[PARTS]),
        pltpu.make_async_copy(win_in, win_ref, in_sem.at[PARTS + 2]),
        pltpu.make_async_copy(cnt_in, cnt_ref, in_sem.at[PARTS + 3]),
        pltpu.make_async_copy(bias_in, bias_ref, in_sem.at[PARTS + 4]),
    ]
    w_copy = pltpu.make_async_copy(w_ref, w_own, in_sem.at[PARTS + 1])
    for copy in kv_in + later_in:
        copy.start()
    w_copy.start()

    def choose(top, crossed, usual):
        word = jnp.int32(0)
        for column in range(8):
            chosen = jnp.where(row == 4, crossed(column), usual(column))
            chosen = jnp.where(row == 0, top(column), chosen)
            word = jnp.where(y == column, chosen, word)
        return word

    peers = choose(lambda c: peer_word(USUAL_PASS, c, True), lambda c: peer_word(CROSSED_PASS, c, False),
                   lambda c: peer_word(USUAL_PASS, c, False))

    is_end = (zl == 0) | (zl == 3)
    is_mid = jnp.logical_not(is_end)
    n1 = 1 + zl // 3
    n2 = 3 - n1
    n3 = 3 - zl
    e1 = (zl - 1) * 3
    m2 = 3 - zl
    e2 = 3 - e1
    first = (row == 0) & (y == 0)
    inner = row > 0

    barrier = pltpu.get_barrier_semaphore()

    def greet(s, h, when=None):
        def signal():
            pl.semaphore_signal(barrier, inc=1, device_id=(s, h), device_id_type=MESH)

        if when is None:
            signal()
        else:
            pl.when(when)(signal)

    for turn in range(1, 8):
        greet(row * 8 + (y + turn) % 8, head, (lax.shift_right_logical(peers, turn) & 1) == 1)
    greet(jnp.where(row == 0, seq + 24, seq - 8), head, row != 4)
    greet(seq + 32, head, row == 0)
    greet(seq - 24, head, (row == 3) | (row == 7))
    greet(seq - 16, head, (row == 2) | (row == 6))
    greet(row * 8, head, (row == 0) & (y >= 1))
    greet(seq, partner)
    greet(seq, n1 * 2 + core, is_end)
    greet(seq, n2 * 2 + core, is_end)
    for d in range(1, 4):
        greet(seq, ((zl + d) % 4) * 2 + core, is_mid)

    def count(flag):
        return jnp.where(flag, 1, 0)

    expect = 3 + count(is_mid) + lax.shift_right_logical(peers, 8) + count(row < 7)
    expect = expect + jnp.where(row == 0, 2, 0) + jnp.where(row == 4, 3, 0) + jnp.where(first, 7, 0)
    with jax.named_scope("greet"):
        pl.semaphore_wait(barrier, expect)

    @pl.when(row == 4)
    def _():
        pl.semaphore_signal(ready, inc=1, device_id=(seq - 32, head), device_id_type=MESH)

    passed = [
        choose(lambda c, i=i: pass_word(USUAL_PASS, c, i), lambda c, i=i: pass_word(CROSSED_PASS, c, i),
               lambda c, i=i: pass_word(USUAL_PASS, c, i))
        for i in range(FAN)
    ]
    word = choose(lambda c: packed(TOP[c]), lambda c: packed(CROSSED[c]), lambda c: packed(USUAL[c]))

    for copy in kv_in:
        copy.wait()

    def x_hop(part):
        return remote(kv.at[0, part], kv.at[8, part], x_send.at[part], kv_recv.at[8, part],
                      jnp.where(row == 3, seq - 24, seq + 8), head)

    crossing = row == 0
    passes = (row == 0) | (row == 4)

    def turn_of(slot, i):
        return lax.shift_right_logical(passed[i], 3 * slot) & 7

    def relay_hop(slot, i, part):
        column = (y + turn_of(slot, i)) % 8
        land = slot + column - y
        return remote(kv.at[slot, part], kv.at[land, part], y_send.at[slot, i, part], kv_recv.at[land, part],
                      row * 8 + column, head)

    def cross_hop(part):
        return remote(kv.at[8, part], kv.at[8, part], y_send.at[8, 0, part], kv_recv.at[8, part], seq + 32, head)

    def held(slot):
        return (slot <= y) | inner | (slot == 8)

    def relays(slot, i):
        return (turn_of(slot, i) != 0) & ((slot <= y) | inner)

    sink_src = kv.at[0, 0, pl.ds(0, SINK_PAD), :]
    sink_src_v = kv.at[0, half, pl.ds(0, SINK_PAD), :]

    def sink_hops(keys, values, n, to):
        return [
            remote(keys, sink.at[0], s_send.at[n, 0], s_recv.at[0], to, head),
            remote(values, sink.at[1], s_send.at[n, 1], s_recv.at[1], to, head),
        ]

    forwards = (
        (0, 8, passes),
        (1, 16, passes),
        (2, 24, passes),
        (3, 32, row == 0),
    )

    def pass_sinks(keys, values, chosen):
        for n, offset, flag in forwards[chosen]:
            @pl.when(flag)
            def _(n=n, offset=offset):
                for copy in sink_hops(keys, values, n, seq + offset):
                    copy.start()

    @pl.when(first)
    def _():
        for d in range(1, 8):
            for copy in sink_hops(sink_src, sink_src_v, 3 + d, d):
                copy.start()
        pass_sinks(sink_src, sink_src_v, slice(0, 3))

    @pl.when(row < 7)
    def _():
        for part in range(PARTS):
            x_hop(part).start()

    for i in range(FAN):
        @pl.when(relays(0, i))
        def _(i=i):
            for part in range(PARTS):
                relay_hop(0, i, part).start()

    w_hop = remote(w_ref, w_oth, w_send, w_recv, seq, partner)
    w_hop.start()

    for copy in later_in:
        copy.wait()
    q_f[...] = q_in[...].astype(F32)
    for p in range(2):
        for h in range(HEADS):
            for d in range(4):
                q_f2[pl.ds(p * HALF + h * 96 + d * OUT_TOK, OUT_TOK), :] = q_f[
                    pl.ds((2 * d + p) * OUT_TOK * HEADS + h, OUT_TOK, HEADS), :]
    qs[...] = q_f2[...].astype(BF)

    m_st[...] = jnp.full_like(m_st, NEG)
    l_st[...] = jnp.zeros_like(l_st)
    acc[...] = jnp.zeros_like(acc)
    scale2 = LOG2E / HD ** 0.5

    def column_facts(tile):
        col = tile * LANES + lax.broadcasted_iota(jnp.int32, (1, LANES), 1)
        p = col // HALF
        h = (col % HALF) // 96
        token = (2 * ((col % 96) // OUT_TOK) + p) * OUT_TOK + col % OUT_TOK

        def per_head(ref):
            value = jnp.where(h == 0, ref[0], ref[1])
            value = jnp.where(h == 2, ref[2], value)
            return jnp.where(h == 3, ref[3], value)

        return seq * TOK + token, per_head

    def fold(tile, scores, values):
        lanes = pl.ds(tile * LANES, LANES)
        m_old = m_st[:, lanes]
        m_new = jnp.maximum(m_old, jnp.max(scores, axis=0, keepdims=True))
        weights = jnp.exp2(scores - m_new)
        alpha = jnp.exp2(m_old - m_new)
        m_st[:, lanes] = m_new
        l_st[:, lanes] = l_st[:, lanes] * alpha + jnp.sum(weights, axis=0, keepdims=True)
        mixed = lax.dot_general(values, weights.astype(BF), (((0,), (0,)), ((), ())),
                                preferred_element_type=F32)
        acc[:, lanes] = acc[:, lanes] * alpha + mixed

    def score_tile(tile, keys):
        return lax.dot_general(keys, qs[pl.ds(tile * LANES, LANES), :], (((1,), (1,)), ((), ())),
                               preferred_element_type=F32) * scale2

    def attend(slot):
        keys = kv[slot, :half].reshape(TOK, HD)
        values = kv[slot, half:].reshape(TOK, HD)
        for tile in range(ROWS // LANES):
            pos, per_head = column_facts(tile)
            key_pos = (seq - slot) * TOK + lax.broadcasted_iota(jnp.int32, (TOK, LANES), 0)
            distance = pos - key_pos
            visible = (distance >= 0) & (distance < per_head(win_ref)) & (key_pos >= per_head(cnt_ref))
            fold(tile, jnp.where(visible, score_tile(tile, keys), NEG), values)

    def attend_sinks():
        keys, values = sink[0], sink[1]
        for tile in range(ROWS // LANES):
            pos, per_head = column_facts(tile)
            key_pos = lax.broadcasted_iota(jnp.int32, (SINK_PAD, LANES), 0)
            visible = (pos >= key_pos) & (key_pos < per_head(cnt_ref))
            scores = score_tile(tile, keys) + per_head(bias_ref) * LOG2E
            fold(tile, jnp.where(visible, scores, NEG), values)

    @pl.when(first)
    def _():
        sink[0] = kv[0, 0, :SINK_PAD, :]
        sink[1] = kv[0, half, :SINK_PAD, :]

    def sink_arrival():
        with jax.named_scope("sink_wait"):
            for copy in sink_hops(sink.at[0], sink.at[1], 0, seq):
                copy.wait_recv()

    def kv_arrival(slot, part):
        return remote(kv.at[slot, part], kv.at[slot, part], x_send.at[part], kv_recv.at[slot, part],
                      seq, partner)

    sink_step = jnp.where((row == 0) | (y == 0), 1, 3)

    with jax.named_scope("attend"):
        attend(0)

    def step(k, carry):
        slot = (lax.shift_right_logical(word, 3 * k) & 7) + 1

        @pl.when((k == sink_step) & passes & jnp.logical_not(first))
        def _():
            sink_arrival()
            pass_sinks(sink.at[0], sink.at[1], slice(0, 4))

        @pl.when((k == sink_step) & first)
        def _():
            pass_sinks(sink_src, sink_src_v, slice(3, 4))

        @pl.when(k == 7)
        def _():
            @pl.when(jnp.logical_not(passes))
            def _():
                sink_arrival()

            attend_sinks()

        across = crossing & (slot == 8)

        @pl.when(held(slot))
        def _():
            for part in range(PARTS):
                with jax.named_scope("kv_wait"):
                    kv_arrival(slot, part).wait_recv()

                @pl.when(across)
                def _(part=part):
                    if part == 0:
                        pl.semaphore_wait(ready, 1)
                    cross_hop(part).start()

                for i in range(FAN):
                    @pl.when(relays(slot, i))
                    def _(part=part, i=i):
                        relay_hop(slot, i, part).start()

        @pl.when(seq >= slot)
        def _():
            with jax.named_scope("attend"):
                attend(slot)

        return carry

    lax.fori_loop(0, 8, step, 0)


    for tile in range(ROWS // 128):
        lanes = pl.ds(tile * 128, 128)
        done = acc[:, lanes] / l_st[:, lanes]
        a_buf[lanes, :] = done.T.astype(BF)

    mine = pl.multiple_of(core * HALF, HALF)
    theirs = pl.multiple_of(HALF - core * HALF, HALF)
    a_hop = remote(a_buf.at[pl.ds(theirs, HALF), :], a_oth, a_send, a_recv, seq, partner)
    a_hop.start()

    a_mine = jnp.concatenate(
        [a_buf[pl.ds(pl.multiple_of(mine + h * 96, 96), 96), :] for h in range(HEADS)], axis=1)
    w_copy.wait()

    for j in range(NC):
        cols = pl.ds(j * CN, CN)
        pacc[:, cols] = jnp.dot(a_mine, w_own[:, cols], preferred_element_type=F32)
    with jax.named_scope('a_wait'):
        a_hop.wait_recv()
    with jax.named_scope('w_wait'):
        w_hop.wait_recv()
    a_other = jnp.concatenate([a_oth[pl.ds(h * 96, 96), :] for h in range(HEADS)], axis=1)

    def item(d, j):
        return pacc[pl.ds(pl.multiple_of(d * OUT_TOK, 8), OUT_TOK), pl.ds(j * CN, CN)]

    def z_hop(n, j, to):
        return remote(sbuf.at[n, j], rbuf.at[zl, j], z_send.at[n, j], z_recv.at[zl, j], seq, to * 2 + core)

    def line_hop(n, j):
        return remote(sbuf.at[n, j], relay.at[n, j], z_send.at[n, j], relay_recv.at[n, j], seq, n1 * 2 + core)

    def relay_arrival(n, j):
        return remote(relay.at[n, j], relay.at[n, j], z_send.at[n, j], relay_recv.at[n, j], seq, partner)

    def z_arrival(source, j):
        return remote(rbuf.at[source, j], rbuf.at[source, j], z_send.at[0, j], z_recv.at[source, j], seq, partner)

    for j in range(NC):
        cols = pl.ds(j * CN, CN)
        pacc[:, cols] += jnp.dot(a_other, w_oth[:, cols], preferred_element_type=F32)

        @pl.when(is_end)
        def _(j=j):
            sbuf[0, j] = item(n3, j).astype(BF)
            line_hop(0, j).start()

        @pl.when(is_mid)
        def _(j=j):
            sbuf[2, j] = item(e1, j).astype(BF)
            z_hop(2, j, e1).start()

    @pl.when(is_end)
    def _():
        for j in range(NC):
            sbuf[1, j] = item(n2, j).astype(BF)
            line_hop(1, j).start()
        for j in range(NC):
            sbuf[2, j] = item(n1, j).astype(BF)
            z_hop(2, j, n1).start()

    @pl.when(row < 7)
    def _():
        for part in range(PARTS):
            x_hop(part).wait_send()

    def drain(slot, carry):
        for i in range(FAN):
            @pl.when(relays(slot, i))
            def _(i=i):
                for part in range(PARTS):
                    relay_hop(slot, i, part).wait_send()

        return carry

    lax.fori_loop(0, 9, drain, 0)

    @pl.when(crossing)
    def _():
        for part in range(PARTS):
            cross_hop(part).wait_send()


    for n, offset, flag in forwards:
        @pl.when(flag)
        def _(n=n, offset=offset):
            for copy in sink_hops(sink.at[0], sink.at[1], n, seq + offset):
                copy.wait_send()

    @pl.when(first)
    def _():
        for d in range(1, 8):
            for copy in sink_hops(sink.at[0], sink.at[1], 3 + d, d):
                copy.wait_send()

    w_hop.wait_send()
    a_hop.wait_send()
    @pl.when(is_mid)
    def _():
        for n, to in ((0, e2), (1, m2)):
            for j in range(NC):
                with jax.named_scope("relay_wait"):
                    relay_arrival(n, j).wait_recv()
                sbuf[n, j] = (item(to, j) + relay[n, j].astype(F32)).astype(BF)
                z_hop(n, j, to).start()

    def collect(sources):
        for j in range(NC):
            total = item(zl, j)
            for source in sources:
                with jax.named_scope('z_wait'):
                    z_arrival(source, j).wait_recv()
                total = total + rbuf[source, j].astype(F32)
            o_ref[:, pl.ds(j * CN, CN)] = total.astype(BF)

    @pl.when(is_end)
    def _():
        collect((n1, n2))

    @pl.when(is_mid)
    def _():
        collect((e1, m2))

    for j in range(NC):
        for n in range(3):
            z_hop(n, j, zl).wait_send()


def shards(queries, key_rows, value_rows, windows, sink_counts, sink_bias, out_weight):
    hbm = pl.BlockSpec(memory_space=pltpu.HBM)
    return pl.pallas_call(
        kernel,
        out_shape=pltpu.VMEM((OUT_TOK, D), BF),
        in_specs=[hbm] * 7,
        out_specs=pl.BlockSpec(memory_space=pltpu.VMEM),
        scratch_shapes=[
            pltpu.SMEM((HEADS,), jnp.int32),
            pltpu.SMEM((HEADS,), jnp.int32),
            pltpu.SMEM((HEADS,), F32),
            pltpu.VMEM((9, PARTS, PART_ROWS, HD), BF),
            pltpu.VMEM((2, SINK_PAD, HD), BF),
            pltpu.VMEM((ROWS, HD), BF),
            pltpu.VMEM((ROWS, HD), F32),
            pltpu.VMEM((ROWS, HD), F32),
            pltpu.VMEM((ROWS, HD), BF),
            pltpu.VMEM((KW, D), BF),
            pltpu.VMEM((KW, D), BF),
            pltpu.VMEM((HD, ROWS), F32),
            pltpu.VMEM((1, ROWS), F32),
            pltpu.VMEM((1, ROWS), F32),
            pltpu.VMEM((ROWS, HD), BF),
            pltpu.VMEM((HALF, HD), BF),
            pltpu.VMEM((96, D), F32),
            pltpu.VMEM((3, NC, OUT_TOK, CN), BF),
            pltpu.VMEM((4, NC, OUT_TOK, CN), BF),
            pltpu.VMEM((2, NC, OUT_TOK, CN), BF),
            pltpu.SemaphoreType.DMA((PARTS + 5,)),
            pltpu.SemaphoreType.DMA((PARTS,)),
            pltpu.SemaphoreType.DMA((9, FAN, PARTS)),
            pltpu.SemaphoreType.DMA((9, PARTS)),
            pltpu.SemaphoreType.DMA((11, 2)),
            pltpu.SemaphoreType.DMA((2,)),
            pltpu.SemaphoreType.DMA,
            pltpu.SemaphoreType.DMA,
            pltpu.SemaphoreType.DMA,
            pltpu.SemaphoreType.DMA,
            pltpu.SemaphoreType.DMA((3, NC)),
            pltpu.SemaphoreType.DMA((4, NC)),
            pltpu.SemaphoreType.DMA((2, NC)),
            pltpu.SemaphoreType.REGULAR,
        ],
        compiler_params=pltpu.CompilerParams(
            collective_id=0, has_side_effects=True, vmem_limit_bytes=67043328 - 512 * 1024),
    )(windows, sink_counts, sink_bias, queries.reshape(ROWS, HD), key_rows.reshape(TOK, HD),
      value_rows.reshape(TOK, HD), out_weight)


def solution(mesh):
    return jax.shard_map(
        shards,
        mesh=mesh,
        in_specs=(
            P("seq", "head", None),
            P("seq", "head", None),
            P("seq", "head", None),
            P("head"),
            P("head"),
            P("head"),
            P("head", None),
        ),
        out_specs=P(("seq", "head"), None),
        check_vma=False,
    )
```
